32 devices in a mesh: dp: 4 (over y, z), tp: 8 (over x, core).
Axes of the slice: x: 4, y: 2, z: 2, core: 2. Of those that a mesh axis runs over, the one named last changes fastest.
The devices are a block of a 4x4x8 slice.
Arguments:
- hidden: bfloat16 [24, 8, 4096], P('dp'), parts along dimension 0
- draft_ids: int32 [24, 7], P('dp'), parts along dimension 0
- temperature: float32 [24], P('dp'), parts along dimension 0
- norm_gain: bfloat16 [4096], replicated
- head_weight: bfloat16 [128256, 4096], P('tp')
Outputs:
- output 1: float32 [24, 7], P('dp'), parts along dimension 0
- output 2: float32 [24, 8], P('dp'), parts along dimension 0
- output 3: float32 [24, 8], P('dp'), parts along dimension 0
There are 4 independent parts. The reference program is written for one: setup_inputs(seed, part) draws one part's arguments, and reference() takes and returns one part's arrays. A program takes and returns all parts, laid end to end along the dimension named above; an argument that names none is the same for every part.
All inputs are finite; a program needn't handle non-finite values.
Results may differ from the reference program's by a relative error of at most 0.001.
Values sent between devices are 32-bit elements.
A program may use at most 768 MiB of HBM per device.

```python
import jax
import jax.numpy as jnp
from jax import lax

BATCH_ROWS = 6
DRAFT_LEN = 7
MODEL_DIM = 4096
VOCAB_SIZE = 128256
NORM_EPS = 1e-5


def setup_inputs(seed: int = 0, part: int = 0) -> dict:
    base_key = jax.random.key(seed)
    part_key = jax.random.fold_in(base_key, part)
    key_hidden, key_draft, key_temp = jax.random.split(part_key, 3)
    key_gain, key_head = jax.random.split(jax.random.key(seed + 1), 2)
    hidden = jax.random.normal(key_hidden, (BATCH_ROWS, DRAFT_LEN + 1, MODEL_DIM), jnp.float32).astype(jnp.bfloat16)
    draft_ids = jax.random.randint(key_draft, (BATCH_ROWS, DRAFT_LEN), 0, VOCAB_SIZE, jnp.int32)
    draft_ids = draft_ids.at[0, 0].set(0).at[0, 1].set(VOCAB_SIZE - 1)
    temperature = jax.random.uniform(key_temp, (BATCH_ROWS,), jnp.float32, 0.6, 1.2)
    norm_gain = (1.5 + 0.3 * jax.random.normal(key_gain, (MODEL_DIM,), jnp.float32)).astype(jnp.bfloat16)
    head_weight = (2.0 * MODEL_DIM ** -0.5 * jax.random.normal(key_head, (VOCAB_SIZE, MODEL_DIM), jnp.float32)).astype(jnp.bfloat16)
    return {"hidden": hidden, "draft_ids": draft_ids, "temperature": temperature, "norm_gain": norm_gain, "head_weight": head_weight}


def reference(hidden, draft_ids, temperature, norm_gain, head_weight):
    hidden_f32 = hidden.astype(jnp.float32)
    mean_sq = jnp.mean(hidden_f32 * hidden_f32, axis=-1, keepdims=True)
    normed = (hidden_f32 * lax.rsqrt(mean_sq + NORM_EPS) * norm_gain.astype(jnp.float32)).astype(jnp.bfloat16)

    def per_row(row_args):
        normed_row, draft_row, temp_row = row_args
        logits = jnp.dot(normed_row, head_weight.T, preferred_element_type=jnp.float32) / temp_row
        row_max = jnp.max(logits, axis=-1, keepdims=True)
        shifted = jnp.exp(logits - row_max)
        total = jnp.sum(shifted, axis=-1)
        weighted = jnp.sum(shifted * logits, axis=-1)
        log_norm = row_max[:, 0] + jnp.log(total)
        entropy = log_norm - weighted / total
        picked = jnp.take_along_axis(logits[:DRAFT_LEN], draft_row[:, None], axis=1)[:, 0]
        return picked - log_norm[:DRAFT_LEN], log_norm, entropy

    log_probs, log_norm, entropy = lax.map(per_row, (normed, draft_ids, temperature))
    return log_probs, log_norm, entropy
```

```python
import functools

import jax
import jax.numpy as jnp
from jax import lax
from jax.experimental import pallas as pl
from jax.experimental.pallas import tpu as pltpu
from jax.sharding import PartitionSpec as P

NORM_EPS = 1e-5
TILE = 1024
SLOTS = 5
LANES = 128
LOW = -1e30


def norm_rows(h_ref, gain_ref, g_ref):
    x = h_ref[...].astype(jnp.float32)
    inv = lax.rsqrt(jnp.mean(x * x, axis=-1, keepdims=True) + NORM_EPS)
    gain = gain_ref[...].astype(jnp.float32)
    for k in range(gain.shape[0]):
        cols = slice(k * LANES, (k + 1) * LANES)
        g_ref[:, cols] = (x[:, cols] * inv * gain[k:k + 1, :]).astype(jnp.bfloat16)


def row_tables(draft_ref, temp_ref, dl_ref, it_ref, first, rows, pos):
    batch, drafts = draft_ref.shape
    sub = lax.broadcasted_iota(jnp.int32, (pos, LANES), 0)
    lane = lax.broadcasted_iota(jnp.int32, (pos, LANES), 1)
    none = -(1 << 24)
    for b in range(batch):
        ids = jnp.broadcast_to(draft_ref[b:b + 1, :].astype(jnp.float32), (pos, drafts))
        own = jnp.where(sub[:, :drafts] == lane[:, :drafts], ids, 0.0)
        col = jnp.sum(own, axis=1, keepdims=True).astype(jnp.int32) - first
        col = jnp.broadcast_to(col, (pos, LANES))
        ok = (col >= 0) & (col < rows) & (sub < drafts)
        dl_ref[b * pos:(b + 1) * pos, :] = jnp.where(ok, col, none)
        temps = jnp.broadcast_to(temp_ref[...], (pos, batch))
        temps = jnp.sum(jnp.where(lane[:, :batch] == b, temps, 0.0), axis=1, keepdims=True)
        it_ref[b * pos:(b + 1) * pos, :] = jnp.broadcast_to(1.0 / temps, (pos, LANES))


def fold_tile(z_ref, width, first, valid, it_ref, dl_ref, m_ref, s_ref, t_ref, p_ref):
    lane = lax.broadcasted_iota(jnp.int32, m_ref.shape, 1)
    scale = it_ref[...]
    wanted = dl_ref[...] - first - lane
    cols = []
    for j in range(width // LANES):
        z = z_ref[:, j * LANES:(j + 1) * LANES] * scale
        if (j + 1) * LANES > valid:
            z = jnp.where(lane < valid - j * LANES, z, 2 * LOW)
        cols.append(z)
    m_old = m_ref[...]
    m_new = m_old
    for z in cols:
        m_new = jnp.maximum(m_new, z)
    alpha = jnp.exp(m_old - m_new)
    s = s_ref[...] * alpha
    t = t_ref[...] * alpha
    p = p_ref[...]
    for j, z in enumerate(cols):
        e = jnp.exp(z - m_new)
        s = s + e
        t = t + e * z
        p = p + jnp.where(wanted == j * LANES, z, 0.0)
    m_ref[...] = m_new
    s_ref[...] = s
    t_ref[...] = t
    p_ref[...] = p


def pack(m_ref, s_ref, t_ref, p_ref, batch, pos):
    sub = lax.broadcasted_iota(jnp.int32, (pos, LANES), 0)
    lane = lax.broadcasted_iota(jnp.int32, (pos, LANES), 1)
    diff = lane - sub
    out_row = lax.broadcasted_iota(jnp.int32, (8, LANES), 0)
    packed = jnp.zeros((8, LANES), jnp.float32)
    for b in range(batch):
        rows = pl.ds(b * pos, pos)
        m = m_ref[rows, :]
        top = jnp.max(m, axis=1, keepdims=True)
        w = jnp.exp(m - top)
        s = jnp.sum(s_ref[rows, :] * w, axis=1, keepdims=True)
        t = jnp.sum(t_ref[rows, :] * w, axis=1, keepdims=True)
        p = jnp.sum(p_ref[rows, :], axis=1, keepdims=True)
        v = jnp.where(diff == 0, s, 0.0)
        v = v + jnp.where(diff == 8, t, 0.0)
        v = v + jnp.where(diff == 16, p, 0.0)
        v = v + jnp.where((diff == 64) | (diff == 72), top, 0.0)
        v = jnp.sum(v, axis=0, keepdims=True)
        packed = jnp.where(out_row == b, v, packed)
    return packed


def kernel(tp, batch, pos, h_hbm, draft_hbm, temp_hbm, gain_hbm, w_ref, out_ref,
           h_ref, draft_ref, temp_ref, gain_ref, dl_ref, it_ref, g_ref, w_buf, w_tail, z_ref, m_ref, s_ref, t_ref, p_ref, send_buf, recv_buf,
           in_sem, w_sem, tail_sem, send_sem, recv_sem):
    rows = w_ref.shape[0]
    n_full = rows // TILE
    tail = rows - n_full * TILE
    me = lax.axis_index("tp")

    def fetch(i, slot):
        return pltpu.make_async_copy(
            w_ref.at[pl.ds(pl.multiple_of(i * TILE, TILE), TILE), :], w_buf.at[slot], w_sem.at[slot])

    tail_copy = pltpu.make_async_copy(
        w_ref.at[pl.ds(n_full * TILE, tail), :], w_tail.at[pl.ds(0, tail), :], tail_sem)

    inputs = [pltpu.make_async_copy(src, dst, in_sem.at[i]) for i, (src, dst) in enumerate(
        ((h_hbm, h_ref), (draft_hbm, draft_ref), (temp_hbm, temp_ref), (gain_hbm, gain_ref)))]
    for copy in inputs:
        copy.start()
    for i in range(SLOTS):
        fetch(i, i).start()

    barrier = pltpu.get_barrier_semaphore()
    for k in range(1, tp):
        pl.semaphore_signal(barrier, inc=1, device_id={"tp": lax.rem(me + k, tp)},
                            device_id_type=pl.DeviceIdType.MESH)

    for copy in inputs:
        copy.wait()
    norm_rows(h_ref, gain_ref, g_ref)
    row_tables(draft_ref, temp_ref, dl_ref, it_ref, me * rows, rows, pos)
    m_ref[...] = jnp.full(m_ref.shape, LOW, jnp.float32)
    s_ref[...] = jnp.zeros(s_ref.shape, jnp.float32)
    t_ref[...] = jnp.zeros(t_ref.shape, jnp.float32)
    p_ref[...] = jnp.zeros(p_ref.shape, jnp.float32)
    z_ref[...] = jnp.full(z_ref.shape, 2 * LOW, jnp.float32)
    pad = w_tail.shape[0] - tail
    if pad:
        w_tail[pl.ds(tail, pad), :] = jnp.zeros((pad, w_tail.shape[1]), jnp.bfloat16)

    def dot(w):
        return lax.dot_general(g_ref[...], w, (((1,), (1,)), ((), ())), preferred_element_type=jnp.float32)

    stats = (it_ref, dl_ref, m_ref, s_ref, t_ref, p_ref)

    def step(i, _):
        slot = lax.rem(i, SLOTS)
        fetch(i, slot).wait()
        fold_tile(z_ref, TILE, (i - 1) * TILE, TILE, *stats)
        z_ref[...] = dot(w_buf[slot])

        @pl.when(i + SLOTS < n_full)
        def _():
            fetch(i + SLOTS, slot).start()

        @pl.when(i + SLOTS == n_full)
        def _():
            tail_copy.start()

        return 0

    lax.fori_loop(0, n_full, step, 0)
    fold_tile(z_ref, TILE, (n_full - 1) * TILE, TILE, *stats)
    tail_copy.wait()
    width = w_tail.shape[0]
    z_ref[:, pl.ds(0, width)] = dot(w_tail[...])
    fold_tile(z_ref, width, n_full * TILE, tail, *stats)

    packed = pack(m_ref, s_ref, t_ref, p_ref, batch, pos)
    send_buf[...] = packed
    recv_buf[me] = packed
    pl.semaphore_wait(barrier, tp - 1)
    copies = []
    for k in range(1, tp):
        copy = pltpu.make_async_remote_copy(
            src_ref=send_buf, dst_ref=recv_buf.at[me], send_sem=send_sem.at[k - 1],
            recv_sem=recv_sem.at[k - 1], device_id={"tp": lax.rem(me + k, tp)},
            device_id_type=pl.DeviceIdType.MESH)
        copy.start()
        copies.append(copy)
    for copy in copies:
        copy.wait()

    parts = [recv_buf[k] for k in range(tp)]
    tops = [pltpu.roll(v, 64, 1) for v in parts]
    top = functools.reduce(jnp.maximum, tops)
    acc = jnp.zeros_like(packed)
    for v, m in zip(parts, tops):
        acc = acc + v * jnp.exp(m - top)
    t_al = pltpu.roll(acc, LANES - 8, 1)
    p_al = pltpu.roll(acc, LANES - 16, 1)
    log_norm = top[:, :pos] + jnp.log(acc[:, :pos])
    out_ref[:, 0:pos] = log_norm
    out_ref[:, 8:8 + pos] = log_norm - t_al[:, :pos] / acc[:, :pos]
    out_ref[:, 16:16 + pos] = p_al[:, :pos] - log_norm


def solution(mesh):
    tp = mesh.shape["tp"]

    def local_step(hidden, draft_ids, temperature, norm_gain, head_shard):
        batch, pos, dim = hidden.shape
        rows = head_shard.shape[0]
        n_rows = batch * pos
        tail = rows % TILE
        tail_pad = -(-tail // 256) * 256
        vmem = pl.BlockSpec(memory_space=pltpu.VMEM)
        stat = pltpu.VMEM((n_rows, LANES), jnp.float32)
        out = pl.pallas_call(
            functools.partial(kernel, tp, batch, pos),
            out_shape=jax.ShapeDtypeStruct((8, LANES), jnp.float32),
            in_specs=[pl.BlockSpec(memory_space=pltpu.HBM)] * 5,
            out_specs=vmem,
            scratch_shapes=[
                pltpu.VMEM((n_rows, dim), jnp.bfloat16),
                pltpu.VMEM(draft_ids.shape, jnp.int32),
                pltpu.VMEM((1, batch), jnp.float32),
                pltpu.VMEM((dim // LANES, LANES), jnp.bfloat16),
                pltpu.VMEM((n_rows, LANES), jnp.int32),
                stat,
                pltpu.VMEM((n_rows, dim), jnp.bfloat16),
                pltpu.VMEM((SLOTS, TILE, dim), jnp.bfloat16),
                pltpu.VMEM((tail_pad, dim), jnp.bfloat16),
                pltpu.VMEM((n_rows, TILE), jnp.float32),
                stat, stat, stat, stat,
                pltpu.VMEM((8, LANES), jnp.float32),
                pltpu.VMEM((tp, 8, LANES), jnp.float32),
                pltpu.SemaphoreType.DMA((4,)),
                pltpu.SemaphoreType.DMA((SLOTS,)),
                pltpu.SemaphoreType.DMA,
                pltpu.SemaphoreType.DMA((tp - 1,)),
                pltpu.SemaphoreType.DMA((tp - 1,)),
            ],
            compiler_params=pltpu.CompilerParams(
                collective_id=0, has_side_effects=True, vmem_limit_bytes=60 * 1024 * 1024),
        )(hidden.reshape(n_rows, dim), draft_ids, temperature.reshape(1, batch),
          norm_gain.reshape(dim // LANES, LANES), head_shard)
        return out[:batch, 16:16 + pos - 1], out[:batch, :pos], out[:batch, 8:8 + pos]

    return jax.shard_map(
        local_step,
        mesh=mesh,
        in_specs=(P("dp", None, None), P("dp", None), P("dp"), P(None), P("tp", None)),
        out_specs=(P("dp", None), P("dp", None), P("dp", None)),
        check_vma=False,
    )
```

```python
import functools

import jax
import jax.numpy as jnp
from jax import lax
from jax.experimental import pallas as pl
from jax.experimental.pallas import tpu as pltpu
from jax.sharding import PartitionSpec as P

NORM_EPS = 1e-5
PAIR = True
TILE = 512
SLOTS = 10
OWN_TILES = 9
FORWARD_AT = (4, 6, 8)
LANES = 128
SUBS = 8
LOW = -1e30
MESH = pl.DeviceIdType.MESH


def norm_rows(h_ref, gain_ref, g_ref):
    x = h_ref[...].astype(jnp.float32)
    inv = lax.rsqrt(jnp.mean(x * x, axis=-1, keepdims=True) + NORM_EPS)
    gain = gain_ref[...].astype(jnp.float32)
    batch, pos, _ = g_ref.shape
    for k in range(gain.shape[0]):
        cols = slice(k * LANES, (k + 1) * LANES)
        g = (x[:, cols] * inv * gain[k:k + 1, :]).astype(jnp.bfloat16).astype(jnp.float32)
        for b in range(batch):
            g_ref[b, :, cols] = g[b * pos:(b + 1) * pos, :]


def transpose_rows(sources, gt_ref):
    batch, pos, dim = sources[0].shape
    used = len(sources) * batch * pos
    for k in range(dim // LANES):
        cols = slice(k * LANES, (k + 1) * LANES)
        rows = [src[b, :, cols] for src in sources for b in range(batch)]
        rows.append(jnp.zeros((LANES - used, LANES), jnp.float32))
        gt_ref[cols, :] = jnp.concatenate(rows, axis=0).T.astype(jnp.bfloat16)


def fold_tile(z_ref, width, first, scale, draft, m_ref, s_ref, t_ref, p_ref):
    wanted = draft - first - lax.broadcasted_iota(jnp.int32, (SUBS, LANES), 0)
    count = width // SUBS

    def chunk(r):
        return z_ref[r * SUBS:(r + 1) * SUBS, :] * scale

    ways = 4
    tops = [m_ref[...]] * ways
    m_old = tops[0]
    for r in range(count):
        tops[r % ways] = jnp.maximum(tops[r % ways], chunk(r))
    m_new = functools.reduce(jnp.maximum, tops)
    alpha = jnp.exp(m_old - m_new)
    zero = jnp.zeros_like(m_old)
    s = [s_ref[...] * alpha] + [zero] * (ways - 1)
    t = [t_ref[...] * alpha] + [zero] * (ways - 1)
    p = [p_ref[...]] + [zero] * (ways - 1)
    for r in range(count):
        z = chunk(r)
        e = jnp.exp(z - m_new)
        w = r % ways
        s[w] = s[w] + e
        t[w] = t[w] + e * z
        p[w] = p[w] + jnp.where(wanted == r * SUBS, z, 0.0)
    m_ref[...] = m_new
    s_ref[...] = sum(s[1:], s[0])
    t_ref[...] = sum(t[1:], t[0])
    p_ref[...] = sum(p[1:], p[0])


def kernel(tp, pair, batch, pos, own, half, h_hbm, draft_hbm, temp_hbm, gain_hbm, w_ref, out_ref,
           h_ref, draft_ref, temp_ref, gain_ref, table_ref, other_table_ref, g_ref, other_ref, gt_ref, w_buf, w_tail, z_ref,
           scale_ref, want_ref, m_ref, s_ref, t_ref, p_ref, msg_ref, inbox_ref,
           in_sem, w_sem, tail_sem, send_sem, recv_sem, pass_sem, got_sem, out_sem, msg_sem):
    rows = w_ref.shape[0]
    used = batch * pos
    me = lax.axis_index("tp")
    dp = lax.axis_index("dp")
    mate = dp + 1 - 2 * lax.rem(dp, 2)
    core = lax.rem(me, 2)
    twin = me + 1 - 2 * core
    n_full = own + half // TILE
    tail = half % TILE
    skip = lax.rem(dp, 2) * half if pair else 0

    def own_tile(i, slot):
        start = pl.multiple_of(i * TILE, TILE)
        return pltpu.make_async_copy(w_ref.at[pl.ds(start, TILE), :], w_buf.at[slot], w_sem.at[slot])

    def shared_tile(i, slot):
        start = pl.multiple_of(i * TILE + skip, 16)
        return pltpu.make_async_copy(w_ref.at[pl.ds(start, TILE), :], w_buf.at[slot], w_sem.at[slot])

    tail_start = pl.multiple_of(n_full * TILE + skip, 16)
    tail_copy = pltpu.make_async_copy(w_ref.at[pl.ds(tail_start, tail), :], w_tail, tail_sem)

    inputs = [pltpu.make_async_copy(src, dst, in_sem.at[i]) for i, (src, dst) in enumerate(
        ((h_hbm, h_ref), (draft_hbm, draft_ref), (temp_hbm, temp_ref), (gain_hbm, gain_ref)))]
    for copy in inputs:
        copy.start()
    for i in range(SLOTS):
        (own_tile if i < own else shared_tile)(i, i).start()

    barrier = pltpu.get_barrier_semaphore()
    peers = [{"dp": dp, "tp": lax.rem(me + k, tp)} for k in range(1, tp)]
    if pair:
        peers += [{"dp": mate, "tp": lax.rem(me + k, tp)} for k in range(tp)]
    for peer in peers:
        pl.semaphore_signal(barrier, inc=1, device_id=peer, device_id_type=MESH)

    for copy in inputs:
        copy.wait()
    norm_rows(h_ref, gain_ref, g_ref)

    lane = lax.broadcasted_iota(jnp.int32, (SUBS, LANES), 1)
    sub = lax.broadcasted_iota(jnp.int32, (SUBS, LANES), 0)
    drafts = draft_ref.shape[1]
    table_ref[...] = jnp.zeros((SUBS, LANES), jnp.float32)
    table_ref[0:batch, 0:drafts] = draft_ref[...].astype(jnp.float32)
    temps = jnp.ones((SUBS, LANES), jnp.float32)
    wants = jnp.full((SUBS, LANES), -1.0, jnp.float32)
    for b in range(batch):
        spread = jnp.broadcast_to(temp_ref[:, b:b + 1], (SUBS, LANES))
        ids = pltpu.roll(jnp.broadcast_to(table_ref[b:b + 1, :], (SUBS, LANES)), b * pos, 1)
        after = lane >= b * pos
        temps = jnp.where(after & (lane < b * pos + pos), spread, temps)
        wants = jnp.where(after & (lane < b * pos + drafts), ids, wants)
    table_ref[...] = jnp.where(sub == 0, temps, wants)
    pl.semaphore_wait(barrier, len(peers))

    trades, passes = [], []
    if pair:
        for j in range(batch // 2):
            b = 2 * j + core
            trades.append(pltpu.make_async_remote_copy(
                src_ref=g_ref.at[b], dst_ref=other_ref.at[b], send_sem=send_sem.at[j], recv_sem=recv_sem.at[j],
                device_id={"dp": mate, "tp": me}, device_id_type=MESH))
            passes.append(pltpu.make_async_remote_copy(
                src_ref=other_ref.at[b], dst_ref=other_ref.at[b], send_sem=pass_sem.at[j], recv_sem=got_sem.at[j],
                device_id={"dp": dp, "tp": twin}, device_id_type=MESH))
        trades.append(pltpu.make_async_remote_copy(
            src_ref=table_ref, dst_ref=other_table_ref, send_sem=send_sem.at[batch // 2],
            recv_sem=recv_sem.at[batch // 2], device_id={"dp": mate, "tp": me}, device_id_type=MESH))
        for copy in trades:
            copy.start()

    transpose_rows([g_ref], gt_ref)
    scale_ref[...] = 1.0 / temps
    want_ref[...] = wants.astype(jnp.int32)
    m_ref[...] = jnp.full((SUBS, LANES), LOW, jnp.float32)
    for ref in (s_ref, t_ref, p_ref):
        ref[...] = jnp.zeros((SUBS, LANES), jnp.float32)
    z_ref[...] = jnp.full(z_ref.shape, 2 * LOW, jnp.float32)

    def fold(width, first):
        fold_tile(z_ref, width, first, scale_ref[...], want_ref[...], m_ref, s_ref, t_ref, p_ref)

    def run_tiles(lo, hi, offset, before=None):
        first = me * rows + offset

        def step(i, _):
            slot = lax.rem(i, SLOTS)
            if before is not None:
                before(i)
            own_tile(0, slot).wait()
            fold(TILE, jnp.where(i > lo, first + (i - 1) * TILE, -(1 << 24)))
            z_ref[...] = jnp.dot(w_buf[slot], gt_ref[...], preferred_element_type=jnp.float32)

            @pl.when(i + SLOTS < own)
            def _():
                own_tile(i + SLOTS, slot).start()

            @pl.when((i + SLOTS >= own) & (i + SLOTS < n_full))
            def _():
                shared_tile(i + SLOTS, slot).start()

            @pl.when(i + SLOTS == n_full)
            def _():
                tail_copy.start()

            return 0

        lax.fori_loop(lo, hi, step, 0)
        fold(TILE, first + (hi - 1) * TILE)

    def pass_on(i):
        for j, at in enumerate(FORWARD_AT):
            @pl.when(i == at)
            def _(j=j):
                trades[j].wait_recv()
                passes[j].start()

    if pair:
        run_tiles(0, own, 0, pass_on)
        z_ref[...] = jnp.full(z_ref.shape, 2 * LOW, jnp.float32)
        mine = lane < used
        m_ref[...] = jnp.where(mine, m_ref[...], LOW)
        for ref in (s_ref, t_ref, p_ref):
            ref[...] = jnp.where(mine, ref[...], 0.0)
        trades[-1].wait_recv()
        both = jnp.where(mine, table_ref[...], pltpu.roll(other_table_ref[...], used, 1))
        temps = jnp.broadcast_to(both[0:1, :], (SUBS, LANES))
        wants = jnp.broadcast_to(both[1:2, :], (SUBS, LANES))
        scale_ref[...] = 1.0 / jnp.where(lane < 2 * used, temps, 1.0)
        want_ref[...] = jnp.where(lane < 2 * used, wants, -1.0).astype(jnp.int32)
        for copy in passes:
            copy.wait_recv()
        transpose_rows([g_ref, other_ref], gt_ref)
        run_tiles(own, n_full, skip)
    else:
        run_tiles(0, n_full, 0)

    tail_copy.wait()
    z_ref[0:tail, :] = jnp.dot(w_tail[...], gt_ref[...], preferred_element_type=jnp.float32)
    fold(tail, me * rows + tail_start)

    top = jnp.max(m_ref[...], axis=0, keepdims=True)
    weight = jnp.exp(m_ref[...] - top)
    total = jnp.sum(s_ref[...] * weight, axis=0, keepdims=True)
    weighted = jnp.sum(t_ref[...] * weight, axis=0, keepdims=True)
    picked = jnp.sum(p_ref[...], axis=0, keepdims=True)
    message = jnp.where(sub == 0, top, jnp.where(sub == 1, total, jnp.where(sub == 2, weighted, picked)))
    msg_ref[...] = message
    inbox_ref[me] = message
    sends = []
    for k, peer in enumerate(peers):
        slot = me if k < tp - 1 else me + tp
        sends.append(pltpu.make_async_remote_copy(
            src_ref=msg_ref, dst_ref=inbox_ref.at[slot], send_sem=out_sem.at[k], recv_sem=msg_sem.at[k],
            device_id=peer, device_id_type=MESH))
    for copy in sends:
        copy.start()
    for copy in trades + passes:
        copy.wait_send()
    for copy in sends:
        copy.wait()

    parts = [inbox_ref[k] for k in range(tp)]
    if pair:
        parts += [pltpu.roll(inbox_ref[tp + k], LANES - used, 1) for k in range(tp)]
    top = functools.reduce(jnp.maximum, [v[0:1, :] for v in parts])
    total = jnp.zeros((1, LANES), jnp.float32)
    weighted = total
    picked = total
    for v in parts:
        weight = jnp.exp(v[0:1, :] - top)
        total = total + v[1:2, :] * weight
        weighted = weighted + v[2:3, :] * weight
        picked = picked + v[3:4, :]
    log_norm = top + jnp.log(total)
    entropy = log_norm - weighted / total
    out = jnp.zeros((SUBS, LANES), jnp.float32)
    for n, row in enumerate((log_norm, entropy, picked - log_norm)):
        row = jnp.broadcast_to(row, (SUBS, LANES))
        for b in range(batch):
            here = (sub == b) & (lane >= n * pos) & (lane < (n + 1) * pos)
            out = jnp.where(here, pltpu.roll(row, (n * pos - b * pos) % LANES, 1), out)
    out_ref[...] = out


def solution(mesh):
    tp = mesh.shape["tp"]
    dp = mesh.shape["dp"]

    def local_step(hidden, draft_ids, temperature, norm_gain, head_shard):
        batch, pos, dim = hidden.shape
        rows = head_shard.shape[0]
        n_rows = batch * pos
        pair = PAIR and dp % 2 == 0 and batch % 2 == 0 and 2 * n_rows <= LANES
        own = OWN_TILES if pair else 0
        half = (rows - own * TILE) // (2 if pair else 1)
        sources = tp * (2 if pair else 1)
        row_block = pltpu.VMEM((batch, pos, dim), jnp.float32)
        stat = pltpu.VMEM((SUBS, LANES), jnp.float32)
        dma = pltpu.SemaphoreType.DMA
        hbm = pl.BlockSpec(memory_space=pltpu.HBM)
        small = [hidden.reshape(n_rows, dim), draft_ids, temperature.reshape(1, batch),
                 norm_gain.reshape(dim // LANES, LANES)]
        small = [pltpu.with_memory_space_constraint(x, pltpu.HBM) for x in small]
        out = pl.pallas_call(
            functools.partial(kernel, tp, pair, batch, pos, own, half),
            out_shape=jax.ShapeDtypeStruct((SUBS, LANES), jnp.float32),
            in_specs=[hbm] * 5,
            out_specs=pl.BlockSpec(memory_space=pltpu.VMEM),
            scratch_shapes=[
                pltpu.VMEM((n_rows, dim), jnp.bfloat16),
                pltpu.VMEM(draft_ids.shape, jnp.int32),
                pltpu.VMEM((1, batch), jnp.float32),
                pltpu.VMEM((dim // LANES, LANES), jnp.bfloat16),
                stat,
                stat,
                row_block,
                row_block,
                pltpu.VMEM((dim, LANES), jnp.bfloat16),
                pltpu.VMEM((SLOTS, TILE, dim), jnp.bfloat16),
                pltpu.VMEM((half % TILE, dim), jnp.bfloat16),
                pltpu.VMEM((TILE, LANES), jnp.float32),
                stat,
                pltpu.VMEM((SUBS, LANES), jnp.int32),
                stat, stat, stat, stat,
                stat,
                pltpu.VMEM((sources, SUBS, LANES), jnp.float32),
                dma((4,)),
                dma((SLOTS,)),
                dma,
                dma((batch // 2 + 1,)),
                dma((batch // 2 + 1,)),
                dma((batch // 2,)),
                dma((batch // 2,)),
                dma((sources - 1,)),
                dma((sources - 1,)),
            ],
            compiler_params=pltpu.CompilerParams(
                collective_id=0, has_side_effects=True, vmem_limit_bytes=50 * 1024 * 1024),
        )(*small, head_shard)
        return out[:batch, 2 * pos:3 * pos - 1], out[:batch, :pos], out[:batch, pos:2 * pos]

    return jax.shard_map(
        local_step,
        mesh=mesh,
        in_specs=(P("dp", None, None), P("dp", None), P("dp"), P(None), P("tp", None)),
        out_specs=(P("dp", None), P("dp", None), P("dp", None)),
        check_vma=False,
    )
```

```python
import functools

import jax
import jax.numpy as jnp
from jax import lax
from jax.experimental import pallas as pl
from jax.experimental.pallas import tpu as pltpu
from jax.sharding import PartitionSpec as P

NORM_EPS = 1e-5
PAIR = True
TILE = 512
SLOTS = 4
EARLY = 2
OWN_TILES = 9
FORWARD_AT = (4, 6, 8)
LANES = 128
SUBS = 8
LOW = -1e30
MESH = pl.DeviceIdType.MESH


def norm_rows(h_ref, gain_ref, g_ref):
    x = h_ref[...].astype(jnp.float32)
    inv = lax.rsqrt(jnp.mean(x * x, axis=-1, keepdims=True) + NORM_EPS)
    gain = gain_ref[...].astype(jnp.float32)
    batch, pos, _ = g_ref.shape
    for k in range(gain.shape[0]):
        cols = slice(k * LANES, (k + 1) * LANES)
        g = (x[:, cols] * inv * gain[k:k + 1, :]).astype(jnp.bfloat16).astype(jnp.float32)
        for b in range(batch):
            g_ref[b, :, cols] = g[b * pos:(b + 1) * pos, :]


def transpose_rows(sources, gt_ref):
    batch, pos, dim = sources[0].shape
    used = len(sources) * batch * pos
    for k in range(dim // LANES):
        cols = slice(k * LANES, (k + 1) * LANES)
        rows = [src[b, :, cols] for src in sources for b in range(batch)]
        rows.append(jnp.zeros((LANES - used, LANES), jnp.float32))
        gt_ref[cols, :] = jnp.concatenate(rows, axis=0).T.astype(jnp.bfloat16)


def fold_tile(z_ref, width, first, scale, draft, m_ref, s_ref, t_ref, p_ref):
    wanted = draft - first - lax.broadcasted_iota(jnp.int32, (SUBS, LANES), 0)
    count = width // SUBS

    def chunk(r):
        return z_ref[r * SUBS:(r + 1) * SUBS, :] * scale

    ways = 4
    tops = [m_ref[...]] * ways
    m_old = tops[0]
    for r in range(count):
        tops[r % ways] = jnp.maximum(tops[r % ways], chunk(r))
    m_new = functools.reduce(jnp.maximum, tops)
    alpha = jnp.exp(m_old - m_new)
    zero = jnp.zeros_like(m_old)
    s = [s_ref[...] * alpha] + [zero] * (ways - 1)
    t = [t_ref[...] * alpha] + [zero] * (ways - 1)
    p = [p_ref[...]] + [zero] * (ways - 1)
    for r in range(count):
        z = chunk(r)
        e = jnp.exp(z - m_new)
        w = r % ways
        s[w] = s[w] + e
        t[w] = t[w] + e * z
        p[w] = p[w] + jnp.where(wanted == r * SUBS, z, 0.0)
    m_ref[...] = m_new
    s_ref[...] = sum(s[1:], s[0])
    t_ref[...] = sum(t[1:], t[0])
    p_ref[...] = sum(p[1:], p[0])


def kernel(tp, pair, batch, pos, own, half, h_hbm, draft_hbm, temp_hbm, gain_hbm, w_ref, out_ref,
           h_ref, draft_ref, temp_ref, gain_ref, table_ref, other_table_ref, g_ref, other_ref, gt_ref, w_buf, w_tail, z_ref,
           scale_ref, want_ref, m_ref, s_ref, t_ref, p_ref, msg_ref, inbox_ref,
           in_sem, w_sem, tail_sem, send_sem, recv_sem, pass_sem, got_sem, out_sem, msg_sem):
    rows = w_ref.shape[0]
    used = batch * pos
    me = lax.axis_index("tp")
    dp = lax.axis_index("dp")
    mate = dp + 1 - 2 * lax.rem(dp, 2)
    core = lax.rem(me, 2)
    twin = me + 1 - 2 * core
    n_full = own + half // TILE
    tail = half % TILE
    skip = lax.rem(dp, 2) * half if pair else 0

    def own_tile(i, slot):
        start = pl.multiple_of(i * TILE, TILE)
        return pltpu.make_async_copy(w_ref.at[pl.ds(start, TILE), :], w_buf.at[slot], w_sem.at[slot])

    def shared_tile(i, slot):
        start = pl.multiple_of(i * TILE + skip, 16)
        return pltpu.make_async_copy(w_ref.at[pl.ds(start, TILE), :], w_buf.at[slot], w_sem.at[slot])

    tail_start = pl.multiple_of(n_full * TILE + skip, 16)
    tail_copy = pltpu.make_async_copy(w_ref.at[pl.ds(tail_start, tail), :], w_tail, tail_sem)

    inputs = [pltpu.make_async_copy(src, dst, in_sem.at[i]) for i, (src, dst) in enumerate(
        ((h_hbm, h_ref), (draft_hbm, draft_ref), (temp_hbm, temp_ref), (gain_hbm, gain_ref)))]
    for copy in inputs:
        copy.start()
    for i in range(EARLY):
        (own_tile if i < own else shared_tile)(i, i).start()

    barrier = pltpu.get_barrier_semaphore()
    peers = [{"dp": dp, "tp": lax.rem(me + k, tp)} for k in range(1, tp)]
    if pair:
        peers += [{"dp": mate, "tp": lax.rem(me + k, tp)} for k in range(tp)]
    for peer in peers:
        pl.semaphore_signal(barrier, inc=1, device_id=peer, device_id_type=MESH)

    for copy in inputs:
        copy.wait()
    norm_rows(h_ref, gain_ref, g_ref)

    lane = lax.broadcasted_iota(jnp.int32, (SUBS, LANES), 1)
    sub = lax.broadcasted_iota(jnp.int32, (SUBS, LANES), 0)
    drafts = draft_ref.shape[1]
    table_ref[...] = jnp.zeros((SUBS, LANES), jnp.float32)
    table_ref[0:batch, 0:drafts] = draft_ref[...].astype(jnp.float32)
    temps = jnp.ones((SUBS, LANES), jnp.float32)
    wants = jnp.full((SUBS, LANES), -1.0, jnp.float32)
    for b in range(batch):
        spread = jnp.broadcast_to(temp_ref[:, b:b + 1], (SUBS, LANES))
        ids = pltpu.roll(jnp.broadcast_to(table_ref[b:b + 1, :], (SUBS, LANES)), b * pos, 1)
        after = lane >= b * pos
        temps = jnp.where(after & (lane < b * pos + pos), spread, temps)
        wants = jnp.where(after & (lane < b * pos + drafts), ids, wants)
    table_ref[...] = jnp.where(sub == 0, temps, wants)
    pl.semaphore_wait(barrier, len(peers))

    trades, passes = [], []
    if pair:
        for j in range(batch // 2):
            b = 2 * j + core
            trades.append(pltpu.make_async_remote_copy(
                src_ref=g_ref.at[b], dst_ref=other_ref.at[b], send_sem=send_sem.at[j], recv_sem=recv_sem.at[j],
                device_id={"dp": mate, "tp": me}, device_id_type=MESH))
            passes.append(pltpu.make_async_remote_copy(
                src_ref=other_ref.at[b], dst_ref=other_ref.at[b], send_sem=pass_sem.at[j], recv_sem=got_sem.at[j],
                device_id={"dp": dp, "tp": twin}, device_id_type=MESH))
        trades.append(pltpu.make_async_remote_copy(
            src_ref=table_ref, dst_ref=other_table_ref, send_sem=send_sem.at[batch // 2],
            recv_sem=recv_sem.at[batch // 2], device_id={"dp": mate, "tp": me}, device_id_type=MESH))
        for copy in trades:
            copy.start()

    for i in range(EARLY, SLOTS):
        (own_tile if i < own else shared_tile)(i, i).start()
    transpose_rows([g_ref], gt_ref)
    scale_ref[...] = 1.0 / temps
    want_ref[...] = wants.astype(jnp.int32)
    m_ref[...] = jnp.full((SUBS, LANES), LOW, jnp.float32)
    for ref in (s_ref, t_ref, p_ref):
        ref[...] = jnp.zeros((SUBS, LANES), jnp.float32)
    z_ref[...] = jnp.full(z_ref.shape, 2 * LOW, jnp.float32)

    def fold(width, first):
        fold_tile(z_ref, width, first, scale_ref[...], want_ref[...], m_ref, s_ref, t_ref, p_ref)

    def run_tiles(lo, hi, offset, before=None):
        first = me * rows + offset

        def step(i, _):
            slot = lax.rem(i, SLOTS)
            if before is not None:
                before(i)
            own_tile(0, slot).wait()
            fold(TILE, jnp.where(i > lo, first + (i - 1) * TILE, -(1 << 24)))
            z_ref[...] = jnp.dot(w_buf[slot], gt_ref[...], preferred_element_type=jnp.float32)

            @pl.when(i + SLOTS < own)
            def _():
                own_tile(i + SLOTS, slot).start()

            @pl.when((i + SLOTS >= own) & (i + SLOTS < n_full))
            def _():
                shared_tile(i + SLOTS, slot).start()

            @pl.when(i + SLOTS == n_full)
            def _():
                tail_copy.start()

            return 0

        lax.fori_loop(lo, hi, step, 0)
        fold(TILE, first + (hi - 1) * TILE)

    def pass_on(i):
        for j, at in enumerate(FORWARD_AT):
            @pl.when(i == at)
            def _(j=j):
                trades[j].wait_recv()
                passes[j].start()

    if pair:
        run_tiles(0, own, 0, pass_on)
        z_ref[...] = jnp.full(z_ref.shape, 2 * LOW, jnp.float32)
        mine = lane < used
        m_ref[...] = jnp.where(mine, m_ref[...], LOW)
        for ref in (s_ref, t_ref, p_ref):
            ref[...] = jnp.where(mine, ref[...], 0.0)
        trades[-1].wait_recv()
        both = jnp.where(mine, table_ref[...], pltpu.roll(other_table_ref[...], used, 1))
        temps = jnp.broadcast_to(both[0:1, :], (SUBS, LANES))
        wants = jnp.broadcast_to(both[1:2, :], (SUBS, LANES))
        scale_ref[...] = 1.0 / jnp.where(lane < 2 * used, temps, 1.0)
        want_ref[...] = jnp.where(lane < 2 * used, wants, -1.0).astype(jnp.int32)
        for copy in passes:
            copy.wait_recv()
        transpose_rows([g_ref, other_ref], gt_ref)
        run_tiles(own, n_full, skip)
    else:
        run_tiles(0, n_full, 0)

    tail_copy.wait()
    z_ref[0:tail, :] = jnp.dot(w_tail[...], gt_ref[...], preferred_element_type=jnp.float32)
    fold(tail, me * rows + tail_start)

    top = jnp.max(m_ref[...], axis=0, keepdims=True)
    weight = jnp.exp(m_ref[...] - top)
    total = jnp.sum(s_ref[...] * weight, axis=0, keepdims=True)
    weighted = jnp.sum(t_ref[...] * weight, axis=0, keepdims=True)
    picked = jnp.sum(p_ref[...], axis=0, keepdims=True)
    message = jnp.where(sub == 0, top, jnp.where(sub == 1, total, jnp.where(sub == 2, weighted, picked)))
    msg_ref[...] = message
    inbox_ref[me] = message
    sends = []
    for k, peer in enumerate(peers):
        slot = me if k < tp - 1 else me + tp
        sends.append(pltpu.make_async_remote_copy(
            src_ref=msg_ref, dst_ref=inbox_ref.at[slot], send_sem=out_sem.at[k], recv_sem=msg_sem.at[k],
            device_id=peer, device_id_type=MESH))
    for copy in sends:
        copy.start()
    for copy in trades + passes:
        copy.wait_send()
    for copy in sends:
        copy.wait()

    parts = [inbox_ref[k] for k in range(tp)]
    if pair:
        parts += [pltpu.roll(inbox_ref[tp + k], LANES - used, 1) for k in range(tp)]
    top = functools.reduce(jnp.maximum, [v[0:1, :] for v in parts])
    total = jnp.zeros((1, LANES), jnp.float32)
    weighted = total
    picked = total
    for v in parts:
        weight = jnp.exp(v[0:1, :] - top)
        total = total + v[1:2, :] * weight
        weighted = weighted + v[2:3, :] * weight
        picked = picked + v[3:4, :]
    log_norm = top + jnp.log(total)
    entropy = log_norm - weighted / total
    out = jnp.zeros((SUBS, LANES), jnp.float32)
    for n, row in enumerate((log_norm, entropy, picked - log_norm)):
        row = jnp.broadcast_to(row, (SUBS, LANES))
        for b in range(batch):
            here = (sub == b) & (lane >= n * pos) & (lane < (n + 1) * pos)
            out = jnp.where(here, pltpu.roll(row, (n * pos - b * pos) % LANES, 1), out)
    out_ref[...] = out


def solution(mesh):
    tp = mesh.shape["tp"]
    dp = mesh.shape["dp"]

    def local_step(hidden, draft_ids, temperature, norm_gain, head_shard):
        batch, pos, dim = hidden.shape
        rows = head_shard.shape[0]
        n_rows = batch * pos
        pair = PAIR and dp % 2 == 0 and batch % 2 == 0 and 2 * n_rows <= LANES
        own = OWN_TILES if pair else 0
        half = (rows - own * TILE) // (2 if pair else 1)
        sources = tp * (2 if pair else 1)
        row_block = pltpu.VMEM((batch, pos, dim), jnp.float32)
        stat = pltpu.VMEM((SUBS, LANES), jnp.float32)
        dma = pltpu.SemaphoreType.DMA
        hbm = pl.BlockSpec(memory_space=pltpu.HBM)
        small = [hidden.reshape(n_rows, dim), draft_ids, temperature.reshape(1, batch),
                 norm_gain.reshape(dim // LANES, LANES)]
        small = [pltpu.with_memory_space_constraint(x, pltpu.HBM) for x in small]
        out = pl.pallas_call(
            functools.partial(kernel, tp, pair, batch, pos, own, half),
            out_shape=jax.ShapeDtypeStruct((SUBS, LANES), jnp.float32),
            in_specs=[hbm] * 5,
            out_specs=pl.BlockSpec(memory_space=pltpu.VMEM),
            scratch_shapes=[
                pltpu.VMEM((n_rows, dim), jnp.bfloat16),
                pltpu.VMEM(draft_ids.shape, jnp.int32),
                pltpu.VMEM((1, batch), jnp.float32),
                pltpu.VMEM((dim // LANES, LANES), jnp.bfloat16),
                stat,
                stat,
                row_block,
                row_block,
                pltpu.VMEM((dim, LANES), jnp.bfloat16),
                pltpu.VMEM((SLOTS, TILE, dim), jnp.bfloat16),
                pltpu.VMEM((half % TILE, dim), jnp.bfloat16),
                pltpu.VMEM((TILE, LANES), jnp.float32),
                stat,
                pltpu.VMEM((SUBS, LANES), jnp.int32),
                stat, stat, stat, stat,
                stat,
                pltpu.VMEM((sources, SUBS, LANES), jnp.float32),
                dma((4,)),
                dma((SLOTS,)),
                dma,
                dma((batch // 2 + 1,)),
                dma((batch // 2 + 1,)),
                dma((batch // 2,)),
                dma((batch // 2,)),
                dma((sources - 1,)),
                dma((sources - 1,)),
            ],
            compiler_params=pltpu.CompilerParams(
                collective_id=0, has_side_effects=True, vmem_limit_bytes=50 * 1024 * 1024),
        )(*small, head_shard)
        return out[:batch, 2 * pos:3 * pos - 1], out[:batch, :pos], out[:batch, pos:2 * pos]

    return jax.shard_map(
        local_step,
        mesh=mesh,
        in_specs=(P("dp", None, None), P("dp", None), P("dp"), P(None), P("tp", None)),
        out_specs=(P("dp", None), P("dp", None), P("dp", None)),
        check_vma=False,
    )
```

```python
import functools

import jax
import jax.numpy as jnp
from jax import lax
from jax.experimental import pallas as pl
from jax.experimental.pallas import tpu as pltpu
from jax.sharding import PartitionSpec as P

NORM_EPS = 1e-5
PAIR = True
TILE = 512
SLOTS = 3
EARLY = 1
OWN_TILES = 11
FORWARD_AT = (4, 6, 8)
LANES = 128
SUBS = 8
LOW = -1e30
MESH = pl.DeviceIdType.MESH


def norm_rows(h_ref, gain_ref, g_ref):
    x = h_ref[...].astype(jnp.float32)
    inv = lax.rsqrt(jnp.mean(x * x, axis=-1, keepdims=True) + NORM_EPS)
    gain = gain_ref[...].astype(jnp.float32)
    batch, pos, _ = g_ref.shape
    for k in range(gain.shape[0]):
        cols = slice(k * LANES, (k + 1) * LANES)
        g = (x[:, cols] * inv * gain[k:k + 1, :]).astype(jnp.bfloat16).astype(jnp.float32)
        for b in range(batch):
            g_ref[b, :, cols] = g[b * pos:(b + 1) * pos, :]


def transpose_rows(sources, gt_ref):
    batch, pos, dim = sources[0].shape
    used = len(sources) * batch * pos
    for k in range(dim // LANES):
        cols = slice(k * LANES, (k + 1) * LANES)
        rows = [src[b, :, cols] for src in sources for b in range(batch)]
        rows.append(jnp.zeros((LANES - used, LANES), jnp.float32))
        gt_ref[cols, :] = jnp.concatenate(rows, axis=0).T.astype(jnp.bfloat16)


def fold_tile(z_ref, width, first, scale, draft, m_ref, s_ref, t_ref, p_ref):
    wanted = draft - first - lax.broadcasted_iota(jnp.int32, (SUBS, LANES), 0)
    count = width // SUBS

    def chunk(r):
        return z_ref[r * SUBS:(r + 1) * SUBS, :] * scale

    ways = 4
    tops = [m_ref[...]] * ways
    m_old = tops[0]
    for r in range(count):
        tops[r % ways] = jnp.maximum(tops[r % ways], chunk(r))
    m_new = functools.reduce(jnp.maximum, tops)
    alpha = jnp.exp(m_old - m_new)
    zero = jnp.zeros_like(m_old)
    s = [s_ref[...] * alpha] + [zero] * (ways - 1)
    t = [t_ref[...] * alpha] + [zero] * (ways - 1)
    p = [p_ref[...]] + [zero] * (ways - 1)
    for r in range(count):
        z = chunk(r)
        e = jnp.exp(z - m_new)
        w = r % ways
        s[w] = s[w] + e
        t[w] = t[w] + e * z
        p[w] = p[w] + jnp.where(wanted == r * SUBS, z, 0.0)
    m_ref[...] = m_new
    s_ref[...] = sum(s[1:], s[0])
    t_ref[...] = sum(t[1:], t[0])
    p_ref[...] = sum(p[1:], p[0])


def kernel(tp, pair, batch, pos, own, half, h_hbm, draft_hbm, temp_hbm, gain_hbm, w_ref, out_ref,
           h_ref, draft_ref, temp_ref, gain_ref, table_ref, other_table_ref, g_ref, other_ref, gt_ref, w_buf, w_tail, z_ref,
           scale_ref, want_ref, m_ref, s_ref, t_ref, p_ref, msg_ref, inbox_ref,
           in_sem, w_sem, tail_sem, send_sem, recv_sem, pass_sem, got_sem, out_sem, msg_sem):
    rows = w_ref.shape[0]
    used = batch * pos
    me = lax.axis_index("tp")
    dp = lax.axis_index("dp")
    mate = dp + 1 - 2 * lax.rem(dp, 2)
    core = lax.rem(me, 2)
    twin = me + 1 - 2 * core
    n_full = own + half // TILE
    tail = half % TILE
    skip = lax.rem(dp, 2) * half if pair else 0

    def own_tile(i, slot):
        start = pl.multiple_of(i * TILE, TILE)
        return pltpu.make_async_copy(w_ref.at[pl.ds(start, TILE), :], w_buf.at[slot], w_sem.at[slot])

    def shared_tile(i, slot):
        start = pl.multiple_of(i * TILE + skip, 16)
        return pltpu.make_async_copy(w_ref.at[pl.ds(start, TILE), :], w_buf.at[slot], w_sem.at[slot])

    tail_start = pl.multiple_of(n_full * TILE + skip, 16)
    tail_copy = pltpu.make_async_copy(w_ref.at[pl.ds(tail_start, tail), :], w_tail, tail_sem)

    inputs = [pltpu.make_async_copy(src, dst, in_sem.at[i]) for i, (src, dst) in enumerate(
        ((h_hbm, h_ref), (draft_hbm, draft_ref), (temp_hbm, temp_ref), (gain_hbm, gain_ref)))]
    for copy in inputs:
        copy.start()
    for i in range(EARLY):
        (own_tile if i < own else shared_tile)(i, i).start()

    barrier = pltpu.get_barrier_semaphore()
    peers = [{"dp": dp, "tp": lax.rem(me + k, tp)} for k in range(1, tp)]
    if pair:
        peers += [{"dp": mate, "tp": lax.rem(me + k, tp)} for k in range(tp)]
    for peer in peers:
        pl.semaphore_signal(barrier, inc=1, device_id=peer, device_id_type=MESH)

    for copy in inputs:
        copy.wait()
    norm_rows(h_ref, gain_ref, g_ref)

    lane = lax.broadcasted_iota(jnp.int32, (SUBS, LANES), 1)
    sub = lax.broadcasted_iota(jnp.int32, (SUBS, LANES), 0)
    drafts = draft_ref.shape[1]
    table_ref[...] = jnp.zeros((SUBS, LANES), jnp.float32)
    table_ref[0:batch, 0:drafts] = draft_ref[...].astype(jnp.float32)
    temps = jnp.ones((SUBS, LANES), jnp.float32)
    wants = jnp.full((SUBS, LANES), -1.0, jnp.float32)
    for b in range(batch):
        spread = jnp.broadcast_to(temp_ref[:, b:b + 1], (SUBS, LANES))
        ids = pltpu.roll(jnp.broadcast_to(table_ref[b:b + 1, :], (SUBS, LANES)), b * pos, 1)
        after = lane >= b * pos
        temps = jnp.where(after & (lane < b * pos + pos), spread, temps)
        wants = jnp.where(after & (lane < b * pos + drafts), ids, wants)
    table_ref[...] = jnp.where(sub == 0, temps, wants)
    pl.semaphore_wait(barrier, len(peers))

    trades, passes = [], []
    if pair:
        for j in range(batch // 2):
            b = 2 * j + core
            trades.append(pltpu.make_async_remote_copy(
                src_ref=g_ref.at[b], dst_ref=other_ref.at[b], send_sem=send_sem.at[j], recv_sem=recv_sem.at[j],
                device_id={"dp": mate, "tp": me}, device_id_type=MESH))
            passes.append(pltpu.make_async_remote_copy(
                src_ref=other_ref.at[b], dst_ref=other_ref.at[b], send_sem=pass_sem.at[j], recv_sem=got_sem.at[j],
                device_id={"dp": dp, "tp": twin}, device_id_type=MESH))
        trades.append(pltpu.make_async_remote_copy(
            src_ref=table_ref, dst_ref=other_table_ref, send_sem=send_sem.at[batch // 2],
            recv_sem=recv_sem.at[batch // 2], device_id={"dp": mate, "tp": me}, device_id_type=MESH))
        for copy in trades:
            copy.start()

    for i in range(EARLY, SLOTS):
        (own_tile if i < own else shared_tile)(i, i).start()
    transpose_rows([g_ref], gt_ref)
    scale_ref[...] = 1.0 / temps
    want_ref[...] = wants.astype(jnp.int32)
    m_ref[...] = jnp.full((SUBS, LANES), LOW, jnp.float32)
    for ref in (s_ref, t_ref, p_ref):
        ref[...] = jnp.zeros((SUBS, LANES), jnp.float32)
    z_ref[...] = jnp.full(z_ref.shape, 2 * LOW, jnp.float32)

    def fold(width, first):
        fold_tile(z_ref, width, first, scale_ref[...], want_ref[...], m_ref, s_ref, t_ref, p_ref)

    def run_tiles(lo, hi, offset, before=None):
        first = me * rows + offset

        def step(i, _):
            slot = lax.rem(i, SLOTS)
            if before is not None:
                before(i)
            own_tile(0, slot).wait()
            fold(TILE, jnp.where(i > lo, first + (i - 1) * TILE, -(1 << 24)))
            z_ref[...] = jnp.dot(w_buf[slot], gt_ref[...], preferred_element_type=jnp.float32)

            @pl.when(i + SLOTS < own)
            def _():
                own_tile(i + SLOTS, slot).start()

            @pl.when((i + SLOTS >= own) & (i + SLOTS < n_full))
            def _():
                shared_tile(i + SLOTS, slot).start()

            @pl.when(i + SLOTS == n_full)
            def _():
                tail_copy.start()

            return 0

        lax.fori_loop(lo, hi, step, 0)
        fold(TILE, first + (hi - 1) * TILE)

    def pass_on(i):
        for j, at in enumerate(FORWARD_AT):
            @pl.when(i == at)
            def _(j=j):
                trades[j].wait_recv()
                passes[j].start()

    if pair:
        run_tiles(0, own, 0, pass_on)
        z_ref[...] = jnp.full(z_ref.shape, 2 * LOW, jnp.float32)
        mine = lane < used
        m_ref[...] = jnp.where(mine, m_ref[...], LOW)
        for ref in (s_ref, t_ref, p_ref):
            ref[...] = jnp.where(mine, ref[...], 0.0)
        trades[-1].wait_recv()
        both = jnp.where(mine, table_ref[...], pltpu.roll(other_table_ref[...], used, 1))
        temps = jnp.broadcast_to(both[0:1, :], (SUBS, LANES))
        wants = jnp.broadcast_to(both[1:2, :], (SUBS, LANES))
        scale_ref[...] = 1.0 / jnp.where(lane < 2 * used, temps, 1.0)
        want_ref[...] = jnp.where(lane < 2 * used, wants, -1.0).astype(jnp.int32)
        for copy in passes:
            copy.wait_recv()
        transpose_rows([g_ref, other_ref], gt_ref)
        run_tiles(own, n_full, skip)
    else:
        run_tiles(0, n_full, 0)

    tail_copy.wait()
    z_ref[0:tail, :] = jnp.dot(w_tail[...], gt_ref[...], preferred_element_type=jnp.float32)
    fold(tail, me * rows + tail_start)

    top = jnp.max(m_ref[...], axis=0, keepdims=True)
    weight = jnp.exp(m_ref[...] - top)
    total = jnp.sum(s_ref[...] * weight, axis=0, keepdims=True)
    weighted = jnp.sum(t_ref[...] * weight, axis=0, keepdims=True)
    picked = jnp.sum(p_ref[...], axis=0, keepdims=True)
    message = jnp.where(sub == 0, top, jnp.where(sub == 1, total, jnp.where(sub == 2, weighted, picked)))
    msg_ref[...] = message
    inbox_ref[me] = message
    sends = []
    for k, peer in enumerate(peers):
        slot = me if k < tp - 1 else me + tp
        sends.append(pltpu.make_async_remote_copy(
            src_ref=msg_ref, dst_ref=inbox_ref.at[slot], send_sem=out_sem.at[k], recv_sem=msg_sem.at[k],
            device_id=peer, device_id_type=MESH))
    for copy in sends:
        copy.start()
    for copy in trades + passes:
        copy.wait_send()
    for copy in sends:
        copy.wait()

    parts = [inbox_ref[k] for k in range(tp)]
    if pair:
        parts += [pltpu.roll(inbox_ref[tp + k], LANES - used, 1) for k in range(tp)]
    top = functools.reduce(jnp.maximum, [v[0:1, :] for v in parts])
    total = jnp.zeros((1, LANES), jnp.float32)
    weighted = total
    picked = total
    for v in parts:
        weight = jnp.exp(v[0:1, :] - top)
        total = total + v[1:2, :] * weight
        weighted = weighted + v[2:3, :] * weight
        picked = picked + v[3:4, :]
    log_norm = top + jnp.log(total)
    entropy = log_norm - weighted / total
    out = jnp.zeros((SUBS, LANES), jnp.float32)
    for n, row in enumerate((log_norm, entropy, picked - log_norm)):
        row = jnp.broadcast_to(row, (SUBS, LANES))
        for b in range(batch):
            here = (sub == b) & (lane >= n * pos) & (lane < (n + 1) * pos)
            out = jnp.where(here, pltpu.roll(row, (n * pos - b * pos) % LANES, 1), out)
    out_ref[...] = out


def spread(packed_ref, lp_ref, lse_ref, ent_ref):
    batch, pos = lse_ref.shape
    packed = packed_ref[...]
    lse_ref[...] = packed[:batch, :pos]
    ent_ref[...] = packed[:batch, pos:2 * pos]
    lp_ref[...] = packed[:batch, 2 * pos:3 * pos - 1]


def solution(mesh):
    tp = mesh.shape["tp"]
    dp = mesh.shape["dp"]

    def local_step(hidden, draft_ids, temperature, norm_gain, head_shard):
        batch, pos, dim = hidden.shape
        rows = head_shard.shape[0]
        n_rows = batch * pos
        pair = PAIR and dp % 2 == 0 and batch % 2 == 0 and 2 * n_rows <= LANES
        own = OWN_TILES if pair else 0
        half = (rows - own * TILE) // (2 if pair else 1)
        sources = tp * (2 if pair else 1)
        row_block = pltpu.VMEM((batch, pos, dim), jnp.float32)
        stat = pltpu.VMEM((SUBS, LANES), jnp.float32)
        dma = pltpu.SemaphoreType.DMA
        hbm = pl.BlockSpec(memory_space=pltpu.HBM)
        small = [hidden.reshape(n_rows, dim), draft_ids, temperature.reshape(1, batch),
                 norm_gain.reshape(dim // LANES, LANES)]
        small = [pltpu.with_memory_space_constraint(x, pltpu.HBM) for x in small]
        out = pl.pallas_call(
            functools.partial(kernel, tp, pair, batch, pos, own, half),
            out_shape=jax.ShapeDtypeStruct((SUBS, LANES), jnp.float32),
            in_specs=[hbm] * 5,
            out_specs=pl.BlockSpec(memory_space=pltpu.VMEM),
            scratch_shapes=[
                pltpu.VMEM((n_rows, dim), jnp.bfloat16),
                pltpu.VMEM(draft_ids.shape, jnp.int32),
                pltpu.VMEM((1, batch), jnp.float32),
                pltpu.VMEM((dim // LANES, LANES), jnp.bfloat16),
                stat,
                stat,
                row_block,
                row_block,
                pltpu.VMEM((dim, LANES), jnp.bfloat16),
                pltpu.VMEM((SLOTS, TILE, dim), jnp.bfloat16),
                pltpu.VMEM((half % TILE, dim), jnp.bfloat16),
                pltpu.VMEM((TILE, LANES), jnp.float32),
                stat,
                pltpu.VMEM((SUBS, LANES), jnp.int32),
                stat, stat, stat, stat,
                stat,
                pltpu.VMEM((sources, SUBS, LANES), jnp.float32),
                dma((4,)),
                dma((SLOTS,)),
                dma,
                dma((batch // 2 + 1,)),
                dma((batch // 2 + 1,)),
                dma((batch // 2,)),
                dma((batch // 2,)),
                dma((sources - 1,)),
                dma((sources - 1,)),
            ],
            compiler_params=pltpu.CompilerParams(
                collective_id=0, has_side_effects=True, vmem_limit_bytes=50 * 1024 * 1024),
        )(*small, head_shard)
        vmem = pl.BlockSpec(memory_space=pltpu.VMEM)
        shapes = ((batch, pos - 1), (batch, pos), (batch, pos))
        return pl.pallas_call(
            spread,
            out_shape=tuple(jax.ShapeDtypeStruct(shape, jnp.float32) for shape in shapes),
            in_specs=[vmem],
            out_specs=(vmem, vmem, vmem),
            compiler_params=pltpu.CompilerParams(vmem_limit_bytes=1 << 20),
        )(out)

    return jax.shard_map(
        local_step,
        mesh=mesh,
        in_specs=(P("dp", None, None), P("dp", None), P("dp"), P(None), P("tp", None)),
        out_specs=(P("dp", None), P("dp", None), P("dp", None)),
        check_vma=False,
    )
```

```python
import functools

import jax
import jax.numpy as jnp
from jax import lax
from jax.experimental import pallas as pl
from jax.experimental.pallas import tpu as pltpu
from jax.sharding import PartitionSpec as P

NORM_EPS = 1e-5
PAIR = True
TILE = 512
SLOTS = 4
EARLY = 2
OWN_TILES = 9
BIG = 2 * TILE
BIG_SLOTS = 3
FORWARD_AT = (4, 6, 8)
LANES = 128
SUBS = 8
LOW = -1e30
MESH = pl.DeviceIdType.MESH


def norm_rows(h_ref, gain_ref, g_ref):
    x = h_ref[...].astype(jnp.float32)
    inv = lax.rsqrt(jnp.mean(x * x, axis=-1, keepdims=True) + NORM_EPS)
    gain = gain_ref[...].astype(jnp.float32)
    batch, pos, _ = g_ref.shape
    for k in range(gain.shape[0]):
        cols = slice(k * LANES, (k + 1) * LANES)
        g = (x[:, cols] * inv * gain[k:k + 1, :]).astype(jnp.bfloat16).astype(jnp.float32)
        for b in range(batch):
            g_ref[b, :, cols] = g[b * pos:(b + 1) * pos, :]


def transpose_rows(sources, gt_ref):
    batch, pos, dim = sources[0].shape
    used = len(sources) * batch * pos
    for k in range(dim // LANES):
        cols = slice(k * LANES, (k + 1) * LANES)
        rows = [src[b, :, cols] for src in sources for b in range(batch)]
        rows.append(jnp.zeros((LANES - used, LANES), jnp.float32))
        gt_ref[cols, :] = jnp.concatenate(rows, axis=0).T.astype(jnp.bfloat16)


def fold_tile(z_ref, width, first, scale, draft, m_ref, s_ref, t_ref, p_ref):
    wanted = draft - first - lax.broadcasted_iota(jnp.int32, (SUBS, LANES), 0)
    count = width // SUBS

    def chunk(r):
        return z_ref[r * SUBS:(r + 1) * SUBS, :] * scale

    ways = 4
    tops = [m_ref[...]] * ways
    m_old = tops[0]
    for r in range(count):
        tops[r % ways] = jnp.maximum(tops[r % ways], chunk(r))
    m_new = functools.reduce(jnp.maximum, tops)
    alpha = jnp.exp(m_old - m_new)
    zero = jnp.zeros_like(m_old)
    s = [s_ref[...] * alpha] + [zero] * (ways - 1)
    t = [t_ref[...] * alpha] + [zero] * (ways - 1)
    p = [p_ref[...]] + [zero] * (ways - 1)
    for r in range(count):
        z = chunk(r)
        e = jnp.exp(z - m_new)
        w = r % ways
        s[w] = s[w] + e
        t[w] = t[w] + e * z
        p[w] = p[w] + jnp.where(wanted == r * SUBS, z, 0.0)
    m_ref[...] = m_new
    s_ref[...] = sum(s[1:], s[0])
    t_ref[...] = sum(t[1:], t[0])
    p_ref[...] = sum(p[1:], p[0])


def kernel(tp, pair, batch, pos, own, half, h_hbm, draft_hbm, temp_hbm, gain_hbm, w_ref, out_ref,
           h_ref, draft_ref, temp_ref, gain_ref, table_ref, other_table_ref, g_ref, other_ref, gt_ref, w_buf, big_buf, w_tail, z_ref,
           scale_ref, want_ref, m_ref, s_ref, t_ref, p_ref, msg_ref, inbox_ref,
           in_sem, w_sem, big_sem, tail_sem, send_sem, recv_sem, pass_sem, got_sem, out_sem, msg_sem):
    rows = w_ref.shape[0]
    used = batch * pos
    me = lax.axis_index("tp")
    dp = lax.axis_index("dp")
    mate = dp + 1 - 2 * lax.rem(dp, 2)
    core = lax.rem(me, 2)
    twin = me + 1 - 2 * core
    n_big = half // BIG
    tail = half % BIG
    shared = own * TILE + (lax.rem(dp, 2) * half if pair else 0)

    def own_tile(i, slot):
        start = pl.multiple_of(i * TILE, TILE)
        return pltpu.make_async_copy(w_ref.at[pl.ds(start, TILE), :], w_buf.at[slot], w_sem.at[slot])

    def big_piece(i, slot, k):
        start = pl.multiple_of(shared + i * BIG + k * TILE, 16)
        return pltpu.make_async_copy(
            w_ref.at[pl.ds(start, TILE), :], big_buf.at[slot, pl.ds(k * TILE, TILE), :], big_sem.at[slot, k])

    tail_start = pl.multiple_of(shared + n_big * BIG, 16)
    tail_copy = pltpu.make_async_copy(w_ref.at[pl.ds(tail_start, tail), :], w_tail, tail_sem)

    inputs = [pltpu.make_async_copy(src, dst, in_sem.at[i]) for i, (src, dst) in enumerate(
        ((h_hbm, h_ref), (draft_hbm, draft_ref), (temp_hbm, temp_ref), (gain_hbm, gain_ref)))]
    for copy in inputs:
        copy.start()
    if pair:
        for i in range(EARLY):
            own_tile(i, i).start()

    barrier = pltpu.get_barrier_semaphore()
    peers = [{"dp": dp, "tp": lax.rem(me + k, tp)} for k in range(1, tp)]
    if pair:
        peers += [{"dp": mate, "tp": lax.rem(me + k, tp)} for k in range(tp)]
    for peer in peers:
        pl.semaphore_signal(barrier, inc=1, device_id=peer, device_id_type=MESH)

    for copy in inputs:
        copy.wait()
    norm_rows(h_ref, gain_ref, g_ref)

    lane = lax.broadcasted_iota(jnp.int32, (SUBS, LANES), 1)
    sub = lax.broadcasted_iota(jnp.int32, (SUBS, LANES), 0)
    drafts = draft_ref.shape[1]
    table_ref[...] = jnp.zeros((SUBS, LANES), jnp.float32)
    table_ref[0:batch, 0:drafts] = draft_ref[...].astype(jnp.float32)
    temps = jnp.ones((SUBS, LANES), jnp.float32)
    wants = jnp.full((SUBS, LANES), -1.0, jnp.float32)
    for b in range(batch):
        spread = jnp.broadcast_to(temp_ref[:, b:b + 1], (SUBS, LANES))
        ids = pltpu.roll(jnp.broadcast_to(table_ref[b:b + 1, :], (SUBS, LANES)), b * pos, 1)
        after = lane >= b * pos
        temps = jnp.where(after & (lane < b * pos + pos), spread, temps)
        wants = jnp.where(after & (lane < b * pos + drafts), ids, wants)
    table_ref[...] = jnp.where(sub == 0, temps, wants)
    pl.semaphore_wait(barrier, len(peers))

    trades, passes = [], []
    if pair:
        for j in range(batch // 2):
            b = 2 * j + core
            trades.append(pltpu.make_async_remote_copy(
                src_ref=g_ref.at[b], dst_ref=other_ref.at[b], send_sem=send_sem.at[j], recv_sem=recv_sem.at[j],
                device_id={"dp": mate, "tp": me}, device_id_type=MESH))
            passes.append(pltpu.make_async_remote_copy(
                src_ref=other_ref.at[b], dst_ref=other_ref.at[b], send_sem=pass_sem.at[j], recv_sem=got_sem.at[j],
                device_id={"dp": dp, "tp": twin}, device_id_type=MESH))
        trades.append(pltpu.make_async_remote_copy(
            src_ref=table_ref, dst_ref=other_table_ref, send_sem=send_sem.at[batch // 2],
            recv_sem=recv_sem.at[batch // 2], device_id={"dp": mate, "tp": me}, device_id_type=MESH))
        for copy in trades:
            copy.start()

        for i in range(EARLY, SLOTS):
            own_tile(i, i).start()
    else:
        for q in range(SLOTS):
            big_piece(q // 2, q // 2, q % 2).start()
    transpose_rows([g_ref], gt_ref)
    scale_ref[...] = 1.0 / temps
    want_ref[...] = wants.astype(jnp.int32)
    m_ref[...] = jnp.full((SUBS, LANES), LOW, jnp.float32)
    for ref in (s_ref, t_ref, p_ref):
        ref[...] = jnp.zeros((SUBS, LANES), jnp.float32)
    z_ref[...] = jnp.full(z_ref.shape, 2 * LOW, jnp.float32)

    def fold(width, first):
        fold_tile(z_ref, width, first, scale_ref[...], want_ref[...], m_ref, s_ref, t_ref, p_ref)

    none = -(1 << 24)

    def third_tile():
        for i in range(SLOTS // 2, BIG_SLOTS):
            for k in range(2):
                big_piece(i, i, k).start()

    def own_step(i, _):
        slot = lax.rem(i, SLOTS)
        pass_on(i)
        own_tile(0, slot).wait()
        fold(TILE, jnp.where(i > 0, me * rows + (i - 1) * TILE, none))
        z_ref[0:TILE, :] = jnp.dot(w_buf[slot], gt_ref[...], preferred_element_type=jnp.float32)

        @pl.when(i + SLOTS < own)
        def _():
            own_tile(i + SLOTS, slot).start()

        for q in range(SLOTS):
            @pl.when(i == own - SLOTS + q)
            def _(q=q):
                big_piece(q // 2, q // 2, q % 2).start()

        return 0

    def big_step(i, _):
        slot = lax.rem(i, BIG_SLOTS)
        for k in range(2):
            big_piece(0, slot, k).wait()
        fold(BIG, jnp.where(i > 0, me * rows + shared + (i - 1) * BIG, none))
        z_ref[...] = jnp.dot(big_buf[slot], gt_ref[...], preferred_element_type=jnp.float32)

        @pl.when(i + BIG_SLOTS < n_big)
        def _():
            for k in range(2):
                big_piece(i + BIG_SLOTS, slot, k).start()

        @pl.when(i + BIG_SLOTS == n_big)
        def _():
            tail_copy.start()

        return 0

    def pass_on(i):
        for j, at in enumerate(FORWARD_AT):
            @pl.when(i == at)
            def _(j=j):
                trades[j].wait_recv()
                passes[j].start()

    if pair:
        lax.fori_loop(0, own, own_step, 0)
        fold(TILE, me * rows + (own - 1) * TILE)
        z_ref[...] = jnp.full(z_ref.shape, 2 * LOW, jnp.float32)
        mine = lane < used
        m_ref[...] = jnp.where(mine, m_ref[...], LOW)
        for ref in (s_ref, t_ref, p_ref):
            ref[...] = jnp.where(mine, ref[...], 0.0)
        trades[-1].wait_recv()
        both = jnp.where(mine, table_ref[...], pltpu.roll(other_table_ref[...], used, 1))
        temps = jnp.broadcast_to(both[0:1, :], (SUBS, LANES))
        wants = jnp.broadcast_to(both[1:2, :], (SUBS, LANES))
        scale_ref[...] = 1.0 / jnp.where(lane < 2 * used, temps, 1.0)
        want_ref[...] = jnp.where(lane < 2 * used, wants, -1.0).astype(jnp.int32)
        for copy in passes:
            copy.wait_recv()
        third_tile()
        transpose_rows([g_ref, other_ref], gt_ref)

    else:
        third_tile()

    lax.fori_loop(0, n_big, big_step, 0)
    fold(BIG, me * rows + shared + (n_big - 1) * BIG)
    tail_copy.wait()
    z_ref[0:tail, :] = jnp.dot(w_tail[...], gt_ref[...], preferred_element_type=jnp.float32)
    fold(tail, me * rows + tail_start)

    top = jnp.max(m_ref[...], axis=0, keepdims=True)
    weight = jnp.exp(m_ref[...] - top)
    total = jnp.sum(s_ref[...] * weight, axis=0, keepdims=True)
    weighted = jnp.sum(t_ref[...] * weight, axis=0, keepdims=True)
    picked = jnp.sum(p_ref[...], axis=0, keepdims=True)
    message = jnp.where(sub == 0, top, jnp.where(sub == 1, total, jnp.where(sub == 2, weighted, picked)))
    msg_ref[...] = message
    inbox_ref[me] = message
    sends = []
    for k, peer in enumerate(peers):
        slot = me if k < tp - 1 else me + tp
        sends.append(pltpu.make_async_remote_copy(
            src_ref=msg_ref, dst_ref=inbox_ref.at[slot], send_sem=out_sem.at[k], recv_sem=msg_sem.at[k],
            device_id=peer, device_id_type=MESH))
    for copy in sends:
        copy.start()
    for copy in trades + passes:
        copy.wait_send()
    for copy in sends:
        copy.wait()

    parts = [inbox_ref[k] for k in range(tp)]
    if pair:
        parts += [pltpu.roll(inbox_ref[tp + k], LANES - used, 1) for k in range(tp)]
    top = functools.reduce(jnp.maximum, [v[0:1, :] for v in parts])
    total = jnp.zeros((1, LANES), jnp.float32)
    weighted = total
    picked = total
    for v in parts:
        weight = jnp.exp(v[0:1, :] - top)
        total = total + v[1:2, :] * weight
        weighted = weighted + v[2:3, :] * weight
        picked = picked + v[3:4, :]
    log_norm = top + jnp.log(total)
    entropy = log_norm - weighted / total
    out = jnp.zeros((SUBS, LANES), jnp.float32)
    for n, row in enumerate((log_norm, entropy, picked - log_norm)):
        row = jnp.broadcast_to(row, (SUBS, LANES))
        for b in range(batch):
            here = (sub == b) & (lane >= n * pos) & (lane < (n + 1) * pos)
            out = jnp.where(here, pltpu.roll(row, (n * pos - b * pos) % LANES, 1), out)
    out_ref[...] = out


def spread(packed_ref, lp_ref, lse_ref, ent_ref):
    batch, pos = lse_ref.shape
    packed = packed_ref[...]
    lse_ref[...] = packed[:batch, :pos]
    ent_ref[...] = packed[:batch, pos:2 * pos]
    lp_ref[...] = packed[:batch, 2 * pos:3 * pos - 1]


def solution(mesh):
    tp = mesh.shape["tp"]
    dp = mesh.shape["dp"]

    def local_step(hidden, draft_ids, temperature, norm_gain, head_shard):
        batch, pos, dim = hidden.shape
        rows = head_shard.shape[0]
        n_rows = batch * pos
        pair = PAIR and dp % 2 == 0 and batch % 2 == 0 and 2 * n_rows <= LANES
        own = OWN_TILES if pair else 0
        half = (rows - own * TILE) // (2 if pair else 1)
        sources = tp * (2 if pair else 1)
        row_block = pltpu.VMEM((batch, pos, dim), jnp.float32)
        stat = pltpu.VMEM((SUBS, LANES), jnp.float32)
        dma = pltpu.SemaphoreType.DMA
        hbm = pl.BlockSpec(memory_space=pltpu.HBM)
        small = [hidden.reshape(n_rows, dim), draft_ids, temperature.reshape(1, batch),
                 norm_gain.reshape(dim // LANES, LANES)]
        small = [pltpu.with_memory_space_constraint(x, pltpu.HBM) for x in small]
        out = pl.pallas_call(
            functools.partial(kernel, tp, pair, batch, pos, own, half),
            out_shape=jax.ShapeDtypeStruct((SUBS, LANES), jnp.float32),
            in_specs=[hbm] * 5,
            out_specs=pl.BlockSpec(memory_space=pltpu.VMEM),
            scratch_shapes=[
                pltpu.VMEM((n_rows, dim), jnp.bfloat16),
                pltpu.VMEM(draft_ids.shape, jnp.int32),
                pltpu.VMEM((1, batch), jnp.float32),
                pltpu.VMEM((dim // LANES, LANES), jnp.bfloat16),
                stat,
                stat,
                row_block,
                row_block,
                pltpu.VMEM((dim, LANES), jnp.bfloat16),
                pltpu.VMEM((SLOTS, TILE, dim), jnp.bfloat16),
                pltpu.VMEM((BIG_SLOTS, BIG, dim), jnp.bfloat16),
                pltpu.VMEM((half % BIG, dim), jnp.bfloat16),
                pltpu.VMEM((BIG, LANES), jnp.float32),
                stat,
                pltpu.VMEM((SUBS, LANES), jnp.int32),
                stat, stat, stat, stat,
                stat,
                pltpu.VMEM((sources, SUBS, LANES), jnp.float32),
                dma((4,)),
                dma((SLOTS,)),
                dma((BIG_SLOTS, 2)),
                dma,
                dma((batch // 2 + 1,)),
                dma((batch // 2 + 1,)),
                dma((batch // 2,)),
                dma((batch // 2,)),
                dma((sources - 1,)),
                dma((sources - 1,)),
            ],
            compiler_params=pltpu.CompilerParams(
                collective_id=0, has_side_effects=True, vmem_limit_bytes=50 * 1024 * 1024),
        )(*small, head_shard)
        vmem = pl.BlockSpec(memory_space=pltpu.VMEM)
        shapes = ((batch, pos - 1), (batch, pos), (batch, pos))
        return pl.pallas_call(
            spread,
            out_shape=tuple(jax.ShapeDtypeStruct(shape, jnp.float32) for shape in shapes),
            in_specs=[vmem],
            out_specs=(vmem, vmem, vmem),
            compiler_params=pltpu.CompilerParams(vmem_limit_bytes=1 << 20),
        )(out)

    return jax.shard_map(
        local_step,
        mesh=mesh,
        in_specs=(P("dp", None, None), P("dp", None), P("dp"), P(None), P("tp", None)),
        out_specs=(P("dp", None), P("dp", None), P("dp", None)),
        check_vma=False,
    )
```

```python
import functools

import jax
import jax.numpy as jnp
from jax import lax
from jax.experimental import pallas as pl
from jax.experimental.pallas import tpu as pltpu
from jax.sharding import PartitionSpec as P

NORM_EPS = 1e-5
PAIR = True
TILE = 512
SLOTS = 4
EARLY = 1
OWN_TILES = 7
BIG = 2 * TILE
BIG_SLOTS = 3
FORWARD_AT = (3, 5, 6)
LANES = 128
SUBS = 8
LOW = -1e30
MESH = pl.DeviceIdType.MESH


def norm_rows(h_ref, gain_ref, g_ref):
    x = h_ref[...].astype(jnp.float32)
    inv = lax.rsqrt(jnp.mean(x * x, axis=-1, keepdims=True) + NORM_EPS)
    gain = gain_ref[...].astype(jnp.float32)
    batch, pos, _ = g_ref.shape
    for k in range(gain.shape[0]):
        cols = slice(k * LANES, (k + 1) * LANES)
        g = (x[:, cols] * inv * gain[k:k + 1, :]).astype(jnp.bfloat16).astype(jnp.float32)
        for b in range(batch):
            g_ref[b, :, cols] = g[b * pos:(b + 1) * pos, :]


def transpose_rows(sources, gt_ref):
    batch, pos, dim = sources[0].shape
    used = len(sources) * batch * pos
    for k in range(dim // LANES):
        cols = slice(k * LANES, (k + 1) * LANES)
        rows = [src[b, :, cols] for src in sources for b in range(batch)]
        rows.append(jnp.zeros((LANES - used, LANES), jnp.float32))
        gt_ref[cols, :] = jnp.concatenate(rows, axis=0).T.astype(jnp.bfloat16)


def fold_tile(z_ref, width, first, scale, draft, m_ref, s_ref, t_ref, p_ref):
    wanted = draft - first - lax.broadcasted_iota(jnp.int32, (SUBS, LANES), 0)
    count = width // SUBS

    def chunk(r):
        return z_ref[r * SUBS:(r + 1) * SUBS, :] * scale

    ways = 4
    tops = [m_ref[...]] * ways
    m_old = tops[0]
    for r in range(count):
        tops[r % ways] = jnp.maximum(tops[r % ways], chunk(r))
    m_new = functools.reduce(jnp.maximum, tops)
    alpha = jnp.exp(m_old - m_new)
    zero = jnp.zeros_like(m_old)
    s = [s_ref[...] * alpha] + [zero] * (ways - 1)
    t = [t_ref[...] * alpha] + [zero] * (ways - 1)
    p = [p_ref[...]] + [zero] * (ways - 1)
    for r in range(count):
        z = chunk(r)
        e = jnp.exp(z - m_new)
        w = r % ways
        s[w] = s[w] + e
        t[w] = t[w] + e * z
        p[w] = p[w] + jnp.where(wanted == r * SUBS, z, 0.0)
    m_ref[...] = m_new
    s_ref[...] = sum(s[1:], s[0])
    t_ref[...] = sum(t[1:], t[0])
    p_ref[...] = sum(p[1:], p[0])


def kernel(tp, pair, batch, pos, own, half, h_hbm, draft_hbm, temp_hbm, gain_hbm, w_ref, out_ref,
           h_ref, draft_ref, temp_ref, gain_ref, table_ref, other_table_ref, g_ref, other_ref, gt_ref, w_buf, big_buf, w_tail, z_ref,
           scale_ref, want_ref, m_ref, s_ref, t_ref, p_ref, msg_ref, inbox_ref,
           in_sem, w_sem, big_sem, tail_sem, send_sem, recv_sem, pass_sem, got_sem, out_sem, msg_sem):
    rows = w_ref.shape[0]
    used = batch * pos
    me = lax.axis_index("tp")
    dp = lax.axis_index("dp")
    mate = dp + 1 - 2 * lax.rem(dp, 2)
    core = lax.rem(me, 2)
    twin = me + 1 - 2 * core
    n_big = half // BIG
    tail = half % BIG
    shared = own * TILE + (lax.rem(dp, 2) * half if pair else 0)

    def own_tile(i, slot):
        start = pl.multiple_of(i * TILE, TILE)
        return pltpu.make_async_copy(w_ref.at[pl.ds(start, TILE), :], w_buf.at[slot], w_sem.at[slot])

    def big_piece(i, slot, k):
        start = pl.multiple_of(shared + i * BIG + k * TILE, 16)
        return pltpu.make_async_copy(
            w_ref.at[pl.ds(start, TILE), :], big_buf.at[slot, pl.ds(k * TILE, TILE), :], big_sem.at[slot, k])

    tail_start = pl.multiple_of(shared + n_big * BIG, 16)
    tail_copy = pltpu.make_async_copy(w_ref.at[pl.ds(tail_start, tail), :], w_tail, tail_sem)

    inputs = [pltpu.make_async_copy(src, dst, in_sem.at[i]) for i, (src, dst) in enumerate(
        ((h_hbm, h_ref), (draft_hbm, draft_ref), (temp_hbm, temp_ref), (gain_hbm, gain_ref)))]
    for copy in inputs:
        copy.start()
    if pair:
        for i in range(EARLY):
            own_tile(i, i).start()

    barrier = pltpu.get_barrier_semaphore()
    peers = [{"dp": dp, "tp": lax.rem(me + k, tp)} for k in range(1, tp)]
    if pair:
        peers += [{"dp": mate, "tp": lax.rem(me + k, tp)} for k in range(tp)]
    for peer in peers:
        pl.semaphore_signal(barrier, inc=1, device_id=peer, device_id_type=MESH)

    for copy in inputs:
        copy.wait()
    norm_rows(h_ref, gain_ref, g_ref)

    lane = lax.broadcasted_iota(jnp.int32, (SUBS, LANES), 1)
    sub = lax.broadcasted_iota(jnp.int32, (SUBS, LANES), 0)
    drafts = draft_ref.shape[1]
    table_ref[...] = jnp.zeros((SUBS, LANES), jnp.float32)
    table_ref[0:batch, 0:drafts] = draft_ref[...].astype(jnp.float32)
    temps = jnp.ones((SUBS, LANES), jnp.float32)
    wants = jnp.full((SUBS, LANES), -1.0, jnp.float32)
    for b in range(batch):
        spread = jnp.broadcast_to(temp_ref[:, b:b + 1], (SUBS, LANES))
        ids = pltpu.roll(jnp.broadcast_to(table_ref[b:b + 1, :], (SUBS, LANES)), b * pos, 1)
        after = lane >= b * pos
        temps = jnp.where(after & (lane < b * pos + pos), spread, temps)
        wants = jnp.where(after & (lane < b * pos + drafts), ids, wants)
    table_ref[...] = jnp.where(sub == 0, temps, wants)
    pl.semaphore_wait(barrier, len(peers))

    trades, passes = [], []
    if pair:
        for j in range(batch // 2):
            b = 2 * j + core
            trades.append(pltpu.make_async_remote_copy(
                src_ref=g_ref.at[b], dst_ref=other_ref.at[b], send_sem=send_sem.at[j], recv_sem=recv_sem.at[j],
                device_id={"dp": mate, "tp": me}, device_id_type=MESH))
            passes.append(pltpu.make_async_remote_copy(
                src_ref=other_ref.at[b], dst_ref=other_ref.at[b], send_sem=pass_sem.at[j], recv_sem=got_sem.at[j],
                device_id={"dp": dp, "tp": twin}, device_id_type=MESH))
        trades.append(pltpu.make_async_remote_copy(
            src_ref=table_ref, dst_ref=other_table_ref, send_sem=send_sem.at[batch // 2],
            recv_sem=recv_sem.at[batch // 2], device_id={"dp": mate, "tp": me}, device_id_type=MESH))
        for copy in trades:
            copy.start()

        for i in range(EARLY, SLOTS):
            own_tile(i, i).start()
    else:
        for q in range(SLOTS):
            big_piece(q // 2, q // 2, q % 2).start()
    transpose_rows([g_ref], gt_ref)
    scale_ref[...] = 1.0 / temps
    want_ref[...] = wants.astype(jnp.int32)
    m_ref[...] = jnp.full((SUBS, LANES), LOW, jnp.float32)
    for ref in (s_ref, t_ref, p_ref):
        ref[...] = jnp.zeros((SUBS, LANES), jnp.float32)
    z_ref[...] = jnp.full(z_ref.shape, 2 * LOW, jnp.float32)

    def fold(width, first):
        fold_tile(z_ref, width, first, scale_ref[...], want_ref[...], m_ref, s_ref, t_ref, p_ref)

    none = -(1 << 24)

    def run_ahead():
        for i in range(SLOTS // 2, BIG_SLOTS):
            for k in range(2):
                big_piece(i, i, k).start()

    def own_step(i, _):
        slot = lax.rem(i, SLOTS)
        pass_on(i)
        own_tile(0, slot).wait()
        fold(TILE, jnp.where(i > 0, me * rows + (i - 1) * TILE, none))
        z_ref[0:TILE, :] = jnp.dot(w_buf[slot], gt_ref[...], preferred_element_type=jnp.float32)

        @pl.when(i + SLOTS < own)
        def _():
            own_tile(i + SLOTS, slot).start()

        for q in range(SLOTS):
            @pl.when(i == own - SLOTS + q)
            def _(q=q):
                big_piece(q // 2, q // 2, q % 2).start()

        @pl.when(i == own - 1)
        def _():
            run_ahead()

        return 0

    def big_step(i, _):
        slot = lax.rem(i, BIG_SLOTS)
        for k in range(2):
            big_piece(0, slot, k).wait()
        fold(BIG, jnp.where(i > 0, me * rows + shared + (i - 1) * BIG, none))
        z_ref[...] = jnp.dot(big_buf[slot], gt_ref[...], preferred_element_type=jnp.float32)

        @pl.when(i + BIG_SLOTS < n_big)
        def _():
            for k in range(2):
                big_piece(i + BIG_SLOTS, slot, k).start()

        @pl.when(i + BIG_SLOTS == n_big)
        def _():
            tail_copy.start()

        return 0

    def pass_on(i):
        for j, at in enumerate(FORWARD_AT):
            @pl.when(i == at)
            def _(j=j):
                trades[j].wait_recv()
                passes[j].start()

    if pair:
        lax.fori_loop(0, own, own_step, 0)
        fold(TILE, me * rows + (own - 1) * TILE)
        z_ref[...] = jnp.full(z_ref.shape, 2 * LOW, jnp.float32)
        mine = lane < used
        m_ref[...] = jnp.where(mine, m_ref[...], LOW)
        for ref in (s_ref, t_ref, p_ref):
            ref[...] = jnp.where(mine, ref[...], 0.0)
        trades[-1].wait_recv()
        both = jnp.where(mine, table_ref[...], pltpu.roll(other_table_ref[...], used, 1))
        temps = jnp.broadcast_to(both[0:1, :], (SUBS, LANES))
        wants = jnp.broadcast_to(both[1:2, :], (SUBS, LANES))
        scale_ref[...] = 1.0 / jnp.where(lane < 2 * used, temps, 1.0)
        want_ref[...] = jnp.where(lane < 2 * used, wants, -1.0).astype(jnp.int32)
        for copy in passes:
            copy.wait_recv()
        transpose_rows([g_ref, other_ref], gt_ref)

    else:
        run_ahead()

    lax.fori_loop(0, n_big, big_step, 0)
    fold(BIG, me * rows + shared + (n_big - 1) * BIG)
    tail_copy.wait()
    z_ref[0:tail, :] = jnp.dot(w_tail[...], gt_ref[...], preferred_element_type=jnp.float32)
    fold(tail, me * rows + tail_start)

    top = jnp.max(m_ref[...], axis=0, keepdims=True)
    weight = jnp.exp(m_ref[...] - top)
    total = jnp.sum(s_ref[...] * weight, axis=0, keepdims=True)
    weighted = jnp.sum(t_ref[...] * weight, axis=0, keepdims=True)
    picked = jnp.sum(p_ref[...], axis=0, keepdims=True)
    message = jnp.where(sub == 0, top, jnp.where(sub == 1, total, jnp.where(sub == 2, weighted, picked)))
    msg_ref[...] = message
    inbox_ref[me] = message
    sends = []
    for k, peer in enumerate(peers):
        slot = me if k < tp - 1 else me + tp
        sends.append(pltpu.make_async_remote_copy(
            src_ref=msg_ref, dst_ref=inbox_ref.at[slot], send_sem=out_sem.at[k], recv_sem=msg_sem.at[k],
            device_id=peer, device_id_type=MESH))
    for copy in sends:
        copy.start()
    for copy in trades + passes:
        copy.wait_send()
    for copy in sends:
        copy.wait()

    parts = [inbox_ref[k] for k in range(tp)]
    if pair:
        parts += [pltpu.roll(inbox_ref[tp + k], LANES - used, 1) for k in range(tp)]
    top = functools.reduce(jnp.maximum, [v[0:1, :] for v in parts])
    total = jnp.zeros((1, LANES), jnp.float32)
    weighted = total
    picked = total
    for v in parts:
        weight = jnp.exp(v[0:1, :] - top)
        total = total + v[1:2, :] * weight
        weighted = weighted + v[2:3, :] * weight
        picked = picked + v[3:4, :]
    log_norm = top + jnp.log(total)
    entropy = log_norm - weighted / total
    out = jnp.zeros((SUBS, LANES), jnp.float32)
    for n, row in enumerate((log_norm, entropy, picked - log_norm)):
        row = jnp.broadcast_to(row, (SUBS, LANES))
        for b in range(batch):
            here = (sub == b) & (lane >= n * pos) & (lane < (n + 1) * pos)
            out = jnp.where(here, pltpu.roll(row, (n * pos - b * pos) % LANES, 1), out)
    out_ref[...] = out


def spread(packed_ref, lp_ref, lse_ref, ent_ref):
    batch, pos = lse_ref.shape
    packed = packed_ref[...]
    lse_ref[...] = packed[:batch, :pos]
    ent_ref[...] = packed[:batch, pos:2 * pos]
    lp_ref[...] = packed[:batch, 2 * pos:3 * pos - 1]


def solution(mesh):
    tp = mesh.shape["tp"]
    dp = mesh.shape["dp"]

    def local_step(hidden, draft_ids, temperature, norm_gain, head_shard):
        batch, pos, dim = hidden.shape
        rows = head_shard.shape[0]
        n_rows = batch * pos
        pair = PAIR and dp % 2 == 0 and batch % 2 == 0 and 2 * n_rows <= LANES
        own = OWN_TILES if pair else 0
        half = (rows - own * TILE) // (2 if pair else 1)
        sources = tp * (2 if pair else 1)
        row_block = pltpu.VMEM((batch, pos, dim), jnp.float32)
        stat = pltpu.VMEM((SUBS, LANES), jnp.float32)
        dma = pltpu.SemaphoreType.DMA
        hbm = pl.BlockSpec(memory_space=pltpu.HBM)
        small = [hidden.reshape(n_rows, dim), draft_ids, temperature.reshape(1, batch),
                 norm_gain.reshape(dim // LANES, LANES)]
        small = [pltpu.with_memory_space_constraint(x, pltpu.HBM) for x in small]
        out = pl.pallas_call(
            functools.partial(kernel, tp, pair, batch, pos, own, half),
            out_shape=jax.ShapeDtypeStruct((SUBS, LANES), jnp.float32),
            in_specs=[hbm] * 5,
            out_specs=pl.BlockSpec(memory_space=pltpu.VMEM),
            scratch_shapes=[
                pltpu.VMEM((n_rows, dim), jnp.bfloat16),
                pltpu.VMEM(draft_ids.shape, jnp.int32),
                pltpu.VMEM((1, batch), jnp.float32),
                pltpu.VMEM((dim // LANES, LANES), jnp.bfloat16),
                stat,
                stat,
                row_block,
                row_block,
                pltpu.VMEM((dim, LANES), jnp.bfloat16),
                pltpu.VMEM((SLOTS, TILE, dim), jnp.bfloat16),
                pltpu.VMEM((BIG_SLOTS, BIG, dim), jnp.bfloat16),
                pltpu.VMEM((half % BIG, dim), jnp.bfloat16),
                pltpu.VMEM((BIG, LANES), jnp.float32),
                stat,
                pltpu.VMEM((SUBS, LANES), jnp.int32),
                stat, stat, stat, stat,
                stat,
                pltpu.VMEM((sources, SUBS, LANES), jnp.float32),
                dma((4,)),
                dma((SLOTS,)),
                dma((BIG_SLOTS, 2)),
                dma,
                dma((batch // 2 + 1,)),
                dma((batch // 2 + 1,)),
                dma((batch // 2,)),
                dma((batch // 2,)),
                dma((sources - 1,)),
                dma((sources - 1,)),
            ],
            compiler_params=pltpu.CompilerParams(
                collective_id=0, has_side_effects=True, vmem_limit_bytes=50 * 1024 * 1024),
        )(*small, head_shard)
        vmem = pl.BlockSpec(memory_space=pltpu.VMEM)
        shapes = ((batch, pos - 1), (batch, pos), (batch, pos))
        return pl.pallas_call(
            spread,
            out_shape=tuple(jax.ShapeDtypeStruct(shape, jnp.float32) for shape in shapes),
            in_specs=[vmem],
            out_specs=(vmem, vmem, vmem),
            compiler_params=pltpu.CompilerParams(vmem_limit_bytes=1 << 20),
        )(out)

    return jax.shard_map(
        local_step,
        mesh=mesh,
        in_specs=(P("dp", None, None), P("dp", None), P("dp"), P(None), P("tp", None)),
        out_specs=(P("dp", None), P("dp", None), P("dp", None)),
        check_vma=False,
    )
```
